64 devices in a mesh: dp: 4 (over x, y), ep: 16 (over z, core).
Axes of the slice: x: 2, y: 2, z: 8, core: 2. Of those that a mesh axis runs over, the one named last changes fastest.
The devices are a block of a 4x4x8 slice.
Arguments:
- hidden_in: bfloat16 [32768, 2048], P(('dp', 'ep')), parts along dimension 0
- topk_idx: int32 [32768, 6], P(('dp', 'ep')), parts along dimension 0
- norm_gain: bfloat16 [2048], replicated
- w_router: bfloat16 [2048, 64], replicated
- w_sgate: bfloat16 [2048, 1], replicated
- s_gate: bfloat16 [2048, 2816], replicated
- s_up: bfloat16 [2048, 2816], replicated
- s_down: bfloat16 [2816, 2048], replicated
- w_gate: bfloat16 [64, 2048, 1408], P('ep')
- w_up: bfloat16 [64, 2048, 1408], P('ep')
- w_down: bfloat16 [64, 1408, 2048], P('ep')
Outputs:
- output: bfloat16 [32768, 2048], P(('dp', 'ep')), parts along dimension 0
There are 4 independent parts. The reference program is written for one: setup_inputs(seed, part) draws one part's arguments, and reference() takes and returns one part's arrays. A program takes and returns all parts, laid end to end along the dimension named above; an argument that names none is the same for every part.
All inputs are finite; a program needn't handle non-finite values.
Results may differ from the reference program's by a relative error of at most 0.00125.
Values are sent between devices in bfloat16 or wider.
A program may use at most 768 MiB of HBM per device.

```python
import jax
import jax.numpy as jnp
from jax import lax

HIDDEN = 2048
EXPERTS = 64
EXPERT_SLOTS = 64
TOP_K = 6
EXPERT_FF = 1408
SHARED_FF = 2816
TOKENS_DEV = 512
GROUP_SIZE = 16

TOKENS = TOKENS_DEV * GROUP_SIZE
CAPACITY = (5 * TOKENS * TOP_K + 4 * EXPERTS - 1) // (4 * EXPERTS)
LOCAL_MAX = (2 * TOKENS_DEV * TOP_K + EXPERTS - 1) // EXPERTS
HOT_COUNT = EXPERTS // 4


def row_order(sub_key):
    return jax.random.permutation(sub_key, TOKENS_DEV)


def draw_routing(route_key):
    key_perm, key_shift, key_rows, key_cols = jax.random.split(route_key, 4)
    per_dev = TOKENS_DEV * TOP_K
    base_perm = jax.random.permutation(key_perm, EXPERTS)
    shifts = jax.random.randint(key_shift, (GROUP_SIZE,), 0, HOT_COUNT)
    pos_index = jnp.arange(per_dev)
    hot_total = HOT_COUNT * LOCAL_MAX
    rest_total = per_dev - hot_total
    rank_seq = jnp.where(pos_index < hot_total, pos_index // LOCAL_MAX,
                         HOT_COUNT + ((pos_index - hot_total) * (EXPERTS - HOT_COUNT)) // rest_total)
    choice = base_perm[(rank_seq[None, :] + shifts[:, None]) % EXPERTS]
    choice = choice.reshape(GROUP_SIZE, TOP_K, TOKENS_DEV).transpose(0, 2, 1)
    row_perm = jax.vmap(row_order)(jax.random.split(key_rows, GROUP_SIZE))
    choice = jnp.take_along_axis(choice, row_perm[:, :, None], axis=1)
    scores = jax.random.randint(key_cols, (GROUP_SIZE, TOKENS_DEV, TOP_K), 0, 1 << 20) * TOP_K + jnp.arange(TOP_K)
    choice = jnp.take_along_axis(choice, jnp.argsort(scores, axis=2), axis=2)
    return choice.reshape(TOKENS, TOP_K).astype(jnp.int32)


def setup_inputs(seed: int = 0, part: int = 0) -> dict:
    base_key = jax.random.key(seed)
    key_x, key_route = jax.random.split(jax.random.fold_in(base_key, part))
    weight_keys = jax.random.split(base_key, 9)
    in_scale = HIDDEN ** -0.5
    down_scale = (EXPERTS / TOP_K) * EXPERT_FF ** -0.5
    live_mask = (jnp.arange(EXPERT_SLOTS) < EXPERTS).astype(jnp.float32)[:, None, None]
    return {
        'hidden_in': (0.5 * jax.random.normal(key_x, (TOKENS, HIDDEN), jnp.float32)).astype(jnp.bfloat16),
        'topk_idx': draw_routing(key_route),
        'norm_gain': (1.0 + 0.3 * jax.random.normal(weight_keys[0], (HIDDEN,), jnp.float32)).astype(jnp.bfloat16),
        'w_router': (in_scale * jax.random.normal(weight_keys[1], (HIDDEN, EXPERTS), jnp.float32)).astype(jnp.bfloat16),
        'w_sgate': (in_scale * jax.random.normal(weight_keys[2], (HIDDEN, 1), jnp.float32)).astype(jnp.bfloat16),
        's_gate': (in_scale * jax.random.normal(weight_keys[3], (HIDDEN, SHARED_FF), jnp.float32)).astype(jnp.bfloat16),
        's_up': (in_scale * jax.random.normal(weight_keys[4], (HIDDEN, SHARED_FF), jnp.float32)).astype(jnp.bfloat16),
        's_down': (SHARED_FF ** -0.5 * jax.random.normal(weight_keys[5], (SHARED_FF, HIDDEN), jnp.float32)).astype(jnp.bfloat16),
        'w_gate': (in_scale * live_mask * jax.random.normal(weight_keys[6], (EXPERT_SLOTS, HIDDEN, EXPERT_FF), jnp.float32)).astype(jnp.bfloat16),
        'w_up': (in_scale * live_mask * jax.random.normal(weight_keys[7], (EXPERT_SLOTS, HIDDEN, EXPERT_FF), jnp.float32)).astype(jnp.bfloat16),
        'w_down': (down_scale * live_mask * jax.random.normal(weight_keys[8], (EXPERT_SLOTS, EXPERT_FF, HIDDEN), jnp.float32)).astype(jnp.bfloat16),
    }


def rms_norm(hidden_in, norm_gain):
    x_f32 = hidden_in.astype(jnp.float32)
    inv_rms = lax.rsqrt(jnp.mean(x_f32 * x_f32, axis=-1, keepdims=True) + 1e-6)
    return (x_f32 * inv_rms * norm_gain.astype(jnp.float32)).astype(jnp.bfloat16)


def expert_mlp(operands):
    expert_rows, gate_w, up_w, down_w = operands
    expert_act = (jax.nn.silu(jnp.dot(expert_rows, gate_w, preferred_element_type=jnp.float32))
                  * jnp.dot(expert_rows, up_w, preferred_element_type=jnp.float32)).astype(jnp.bfloat16)
    return jnp.dot(expert_act, down_w, preferred_element_type=jnp.float32).astype(jnp.bfloat16)


def reference(hidden_in, topk_idx, norm_gain, w_router, w_sgate, s_gate, s_up, s_down, w_gate, w_up, w_down):
    normed = rms_norm(hidden_in, norm_gain)
    router_probs = jax.nn.softmax(jnp.dot(normed, w_router, preferred_element_type=jnp.float32), axis=-1)
    gate_vals = jnp.take_along_axis(router_probs, topk_idx, axis=1)
    flat_ids = topk_idx.reshape(-1)
    onehot = (flat_ids[:, None] == jnp.arange(EXPERTS)[None, :]).astype(jnp.int32)
    position = jnp.sum((jnp.cumsum(onehot, axis=0) - onehot) * onehot, axis=1)
    slot_pos = jnp.where(position < CAPACITY, flat_ids * CAPACITY + position, EXPERTS * CAPACITY)
    token_of = jnp.arange(TOKENS * TOP_K) // TOP_K
    row_table = jnp.full((EXPERTS * CAPACITY,), TOKENS, jnp.int32).at[slot_pos].set(token_of, mode='drop')
    expert_rows = jnp.take(normed, row_table, axis=0, mode='fill', fill_value=0).reshape(EXPERTS, CAPACITY, HIDDEN)
    results = lax.map(expert_mlp, (expert_rows, w_gate[:EXPERTS], w_up[:EXPERTS], w_down[:EXPERTS]))
    picked = jnp.take(results.reshape(EXPERTS * CAPACITY, HIDDEN), slot_pos, axis=0, mode='fill', fill_value=0)
    picked = picked.reshape(TOKENS, TOP_K, HIDDEN)
    routed = jnp.sum(gate_vals[:, :, None] * picked.astype(jnp.float32), axis=1)
    shared_act = (jax.nn.silu(jnp.dot(normed, s_gate, preferred_element_type=jnp.float32))
                  * jnp.dot(normed, s_up, preferred_element_type=jnp.float32)).astype(jnp.bfloat16)
    shared_val = jnp.dot(shared_act, s_down, preferred_element_type=jnp.float32)
    shared_gate = jax.nn.sigmoid(jnp.dot(normed, w_sgate, preferred_element_type=jnp.float32))
    return (hidden_in.astype(jnp.float32) + routed + shared_gate * shared_val).astype(jnp.bfloat16)
```

```python
import functools

import jax
import jax.numpy as jnp
from jax import lax
from jax.experimental import pallas as pl
from jax.experimental.pallas import tpu as pltpu
from jax.sharding import PartitionSpec as P

CHUNKS = 2
ROW_TILE = 192
F32 = jnp.float32
BF16 = jnp.bfloat16


def rms_norm(hidden_in, norm_gain):
    x_f32 = hidden_in.astype(F32)
    inv_rms = lax.rsqrt(jnp.mean(x_f32 * x_f32, axis=-1, keepdims=True) + 1e-6)
    return (x_f32 * inv_rms * norm_gain.astype(F32)).astype(BF16)


def shared_expert(normed, w_sgate, s_gate, s_up, s_down):
    shared_act = (jax.nn.silu(jnp.dot(normed, s_gate, preferred_element_type=F32))
                  * jnp.dot(normed, s_up, preferred_element_type=F32)).astype(BF16)
    shared_val = jnp.dot(shared_act, s_down, preferred_element_type=F32)
    return jax.nn.sigmoid(jnp.dot(normed, w_sgate, preferred_element_type=F32)) * shared_val


def exclusive_count(flags):
    lead, total = flags.shape
    lanes = 128
    blocks = total // lanes
    grid = flags.astype(BF16).reshape(lead * blocks, lanes)
    upper = (jnp.arange(lanes)[:, None] < jnp.arange(lanes)[None, :]).astype(BF16)
    inner = jnp.dot(grid, upper, preferred_element_type=F32).reshape(lead, blocks, lanes)
    sums = jnp.sum(flags.reshape(lead, blocks, lanes), axis=-1)
    before = (jnp.arange(blocks)[:, None] < jnp.arange(blocks)[None, :]).astype(BF16)
    outer = jnp.dot(sums.astype(BF16), before, preferred_element_type=F32)
    return (inner + outer[:, :, None]).reshape(lead, total)


def ffn_kernel(count_ref, x_ref, gate_ref, up_ref, down_ref, out_ref):
    tiles = pl.num_programs(1)
    filled = lax.div(count_ref[pl.program_id(0)] + (ROW_TILE - 1), ROW_TILE)

    @pl.when(pl.program_id(1) >= tiles - filled)
    def _():
        rows = x_ref[0]
        gate = jnp.dot(rows, gate_ref[0], preferred_element_type=F32)
        up = jnp.dot(rows, up_ref[0], preferred_element_type=F32)
        act = (gate * jax.nn.sigmoid(gate) * up).astype(BF16)
        out_ref[0] = jnp.dot(act, down_ref[0], preferred_element_type=F32).astype(BF16)


def expert_ffn(counts, rows, w_gate, w_up, w_down):
    slots, padded, hidden = rows.shape
    ff = w_gate.shape[2]
    tiles = padded // ROW_TILE

    def row_map(e, r, count_ref):
        filled = lax.div(count_ref[e] + (ROW_TILE - 1), ROW_TILE)
        return e, jnp.maximum(r - (tiles - filled), 0), 0

    def weight_map(e, r, count_ref):
        return e, 0, 0

    return pl.pallas_call(
        ffn_kernel,
        out_shape=jax.ShapeDtypeStruct((slots, padded, hidden), BF16),
        grid_spec=pltpu.PrefetchScalarGridSpec(
            num_scalar_prefetch=1,
            grid=(slots, tiles),
            in_specs=[
                pl.BlockSpec((1, ROW_TILE, hidden), row_map),
                pl.BlockSpec((1, hidden, ff), weight_map),
                pl.BlockSpec((1, hidden, ff), weight_map),
                pl.BlockSpec((1, ff, hidden), weight_map),
            ],
            out_specs=pl.BlockSpec((1, ROW_TILE, hidden), row_map),
        ),
        compiler_params=pltpu.CompilerParams(
            dimension_semantics=("arbitrary", "arbitrary"), vmem_limit_bytes=58 * 1024 * 1024),
        cost_estimate=pl.CostEstimate(
            flops=3 * slots * padded * hidden * ff, bytes_accessed=6 * slots * hidden * ff,
            transcendentals=0),
        name="expert_ffn",
    )(counts, rows, w_gate, w_up, w_down)


def combine_kernel(slots, window, start_ref, count_ref, meta_ref, rows_ref, out_ref):
    source = pl.program_id(0)
    tokens = meta_ref.shape[0]
    padded = rows_ref.shape[1]
    lane = lax.broadcasted_iota(jnp.int32, (tokens, window), 1)
    sub = lax.broadcasted_iota(jnp.int32, (window, 1), 0)
    meta = meta_ref[...]
    for e in range(slots):
        first = lax.div(start_ref[source * slots + e], 16) * 16
        first = pl.multiple_of(jnp.minimum(first, padded - window), 16)
        rows = rows_ref[e, pl.ds(first, window), :]
        rows = jnp.where(sub + first < count_ref[e], rows, jnp.zeros_like(rows))
        wanted = meta[:, e:e + 1].astype(jnp.int32) - first
        pick = (lane == wanted).astype(F32).astype(BF16)
        term = meta[:, slots + e:slots + e + 1] * jnp.dot(pick, rows, preferred_element_type=F32)
        if e == 0:
            out_ref[0] = term
        else:
            out_ref[0] += term


def combine(starts, counts, meta, rows, window, sources):
    slots, padded, hidden = rows.shape
    tokens = meta.shape[0] // sources
    return pl.pallas_call(
        functools.partial(combine_kernel, slots, window),
        out_shape=jax.ShapeDtypeStruct((sources, tokens, hidden), F32),
        grid_spec=pltpu.PrefetchScalarGridSpec(
            num_scalar_prefetch=2,
            grid=(sources,),
            in_specs=[
                pl.BlockSpec((tokens, meta.shape[1]), lambda s, *_: (s, 0)),
                pl.BlockSpec((slots, padded, hidden), lambda s, *_: (0, 0, 0),
                             pipeline_mode=pl.Buffered(1)),
            ],
            out_specs=pl.BlockSpec((1, tokens, hidden), lambda s, *_: (s, 0, 0)),
        ),
        compiler_params=pltpu.CompilerParams(
            dimension_semantics=("arbitrary",), vmem_limit_bytes=48 * 1024 * 1024),
        cost_estimate=pl.CostEstimate(
            flops=2 * sources * tokens * slots * 256 * hidden,
            bytes_accessed=4 * sources * tokens * hidden, transcendentals=0),
        name="combine",
    )(starts, counts, meta, rows)


def solution(mesh):
    group_size = mesh.shape['ep']

    def device_block(hidden_in, topk_idx, norm_gain, w_router, w_sgate, s_gate, s_up, s_down, w_gate, w_up, w_down):
        tok_dev, hidden = hidden_in.shape
        top_k = topk_idx.shape[1]
        experts = w_router.shape[1]
        slots = w_gate.shape[0]
        capacity = (5 * tok_dev * group_size * top_k + 4 * experts - 1) // (4 * experts)
        local_max = (2 * tok_dev * top_k + experts - 1) // experts
        padded = -(-capacity // ROW_TILE) * ROW_TILE
        window = -(-local_max // 16) * 16 + 16
        part = tok_dev // CHUNKS
        my_rank = lax.axis_index('ep')

        normed = rms_norm(hidden_in, norm_gain)
        gathered = [lax.all_gather(normed[c * part:(c + 1) * part], 'ep', tiled=True) for c in range(CHUNKS)]

        logits = lax.dot_general(w_router, normed, (((0,), (1,)), ((), ())), preferred_element_type=F32)
        probs = jax.nn.softmax(logits, axis=0)
        ids = topk_idx.T
        ids_f32 = ids.astype(F32)
        gates = jnp.sum(jnp.where(ids[:, None, :] == jnp.arange(experts)[None, :, None], probs[None], 0.0), axis=1)
        route = lax.all_gather(jnp.concatenate([ids_f32, gates], axis=0), 'ep')
        all_ids, all_gates = route[:, :top_k], route[:, top_k:]

        my_slots = (my_rank * slots + jnp.arange(slots)).astype(F32)
        match = all_ids[None] == my_slots[:, None, None, None]
        hit = jnp.sum(match.astype(F32), axis=2)
        gate = jnp.sum(jnp.where(match, all_gates[None], 0.0), axis=2)
        order = exclusive_count(hit.reshape(slots, group_size * tok_dev)).reshape(hit.shape)
        kept = jnp.where(order < capacity, hit, 0.0)

        partial_sums = []
        for c in range(CHUNKS):
            kept_c = kept[:, :, c * part:(c + 1) * part].reshape(slots, group_size * part)
            gate_c = gate[:, :, c * part:(c + 1) * part].reshape(slots, group_size * part)
            place = exclusive_count(kept_c)
            place = jnp.where(kept_c > 0, place, -1.0)
            per_source = jnp.sum(kept_c.reshape(slots, group_size, part), axis=2).astype(jnp.int32)
            counts = jnp.sum(per_source, axis=1)
            starts = (jnp.cumsum(per_source, axis=1) - per_source).T.reshape(-1)
            meta = jnp.concatenate([place, gate_c], axis=0).T
            token = jnp.arange(group_size * part, dtype=jnp.int32)
            seats = jnp.arange(padded, dtype=jnp.int32).astype(F32)
            table = jnp.sum(jnp.where(place[:, None, :] == seats[None, :, None], token[None, None, :], 0), axis=2)
            rows = gathered[c].at[table.reshape(-1)].get(mode='promise_in_bounds')
            results = expert_ffn(counts, rows.reshape(slots, padded, hidden), w_gate, w_up, w_down)
            partial = combine(starts, counts, meta, results, window, group_size)
            partial_sums.append(partial.reshape(group_size * part, hidden))
        routed = [lax.psum_scatter(p, 'ep', scatter_dimension=0, tiled=True) for p in partial_sums]
        shared_in, _ = lax.optimization_barrier((normed, partial_sums[0]))
        shared_val = shared_expert(shared_in, w_sgate, s_gate, s_up, s_down)
        base = lax.optimization_barrier(hidden_in.astype(F32) + shared_val)
        return (base + jnp.concatenate(routed, axis=0)).astype(BF16)

    row_spec = P(('dp', 'ep'), None)
    full_spec = P(None, None)
    slot_spec = P('ep', None, None)
    in_specs = (row_spec, row_spec, P(None), full_spec, full_spec, full_spec, full_spec, full_spec,
                slot_spec, slot_spec, slot_spec)
    return jax.shard_map(device_block, mesh=mesh, in_specs=in_specs, out_specs=row_spec, check_vma=False)
```

```python
import functools

import jax
import jax.numpy as jnp
from jax import lax
from jax.experimental import pallas as pl
from jax.experimental.pallas import tpu as pltpu
from jax.sharding import PartitionSpec as P

SPLIT = (3, 5)
ROW_TILE = 192
F32 = jnp.float32
BF16 = jnp.bfloat16


def rms_norm(hidden_in, norm_gain):
    x_f32 = hidden_in.astype(F32)
    inv_rms = lax.rsqrt(jnp.mean(x_f32 * x_f32, axis=-1, keepdims=True) + 1e-6)
    return (x_f32 * inv_rms * norm_gain.astype(F32)).astype(BF16), inv_rms


def shared_expert(normed, w_sgate, s_gate, s_up, s_down):
    shared_act = (jax.nn.silu(jnp.dot(normed, s_gate, preferred_element_type=F32))
                  * jnp.dot(normed, s_up, preferred_element_type=F32)).astype(BF16)
    shared_val = jnp.dot(shared_act, s_down, preferred_element_type=F32)
    return jax.nn.sigmoid(jnp.dot(normed, w_sgate, preferred_element_type=F32)) * shared_val


def exclusive_count(flags):
    lead, total = flags.shape
    lanes = 128
    blocks = total // lanes
    grid = flags.astype(BF16).reshape(lead * blocks, lanes)
    upper = (jnp.arange(lanes)[:, None] < jnp.arange(lanes)[None, :]).astype(BF16)
    inner = jnp.dot(grid, upper, preferred_element_type=F32).reshape(lead, blocks, lanes)
    sums = jnp.sum(flags.reshape(lead, blocks, lanes), axis=-1)
    before = (jnp.arange(blocks)[:, None] < jnp.arange(blocks)[None, :]).astype(BF16)
    outer = jnp.dot(sums.astype(BF16), before, preferred_element_type=F32)
    return (inner + outer[:, :, None]).reshape(lead, total)


def pack_kernel(slots, window, start_ref, seat_ref, gain_ref, x_ref, out_ref):
    source = pl.program_id(0)
    tokens = x_ref.shape[0]
    padded = out_ref.shape[1]
    sub = lax.broadcasted_iota(jnp.int32, (window, tokens), 0)
    row = lax.broadcasted_iota(jnp.int32, (window, 1), 0)
    inv_rms = seat_ref[0, slots:slots + 1, :]
    gain = gain_ref[...]
    for e in range(slots):
        start = start_ref[source * slots + e]
        first = pl.multiple_of(jnp.minimum(lax.div(start, 16) * 16, padded - window), 16)
        chosen = sub == seat_ref[0, e:e + 1, :].astype(jnp.int32) - first
        pick = chosen.astype(F32).astype(BF16)
        scale = jnp.sum(jnp.where(chosen, inv_rms, 0.0), axis=1, keepdims=True)
        rows = jnp.dot(pick, x_ref[...], preferred_element_type=F32)
        rows = (rows * scale * gain).astype(BF16)
        old = out_ref[e, pl.ds(first, window), :]
        out_ref[e, pl.ds(first, window), :] = jnp.where(row + first >= start, rows, old)


def pack_rows(starts, seats, gain, x_rows, slots, padded, window, sources):
    hidden = x_rows.shape[1]
    tokens = x_rows.shape[0] // sources
    return pl.pallas_call(
        functools.partial(pack_kernel, slots, window),
        out_shape=jax.ShapeDtypeStruct((slots, padded, hidden), BF16),
        grid_spec=pltpu.PrefetchScalarGridSpec(
            num_scalar_prefetch=1,
            grid=(sources,),
            in_specs=[
                pl.BlockSpec((1,) + seats.shape[1:], lambda s, *_: (s, 0, 0)),
                pl.BlockSpec((1, hidden), lambda s, *_: (0, 0)),
                pl.BlockSpec((tokens, hidden), lambda s, *_: (s, 0)),
            ],
            out_specs=pl.BlockSpec((slots, padded, hidden), lambda s, *_: (0, 0, 0)),
        ),
        compiler_params=pltpu.CompilerParams(
            dimension_semantics=("arbitrary",), vmem_limit_bytes=52 * 1024 * 1024),
        cost_estimate=pl.CostEstimate(
            flops=2 * sources * tokens * slots * 256 * hidden,
            bytes_accessed=2 * sources * tokens * hidden, transcendentals=0),
        name="pack_rows",
    )(starts, seats, gain, x_rows)


def ffn_kernel(count_ref, x_ref, gate_ref, up_ref, down_ref, out_ref):
    tiles = pl.num_programs(1)
    filled = lax.div(count_ref[pl.program_id(0)] + (ROW_TILE - 1), ROW_TILE)

    @pl.when(pl.program_id(1) >= tiles - filled)
    def _():
        rows = x_ref[0]
        gate = jnp.dot(rows, gate_ref[0], preferred_element_type=F32)
        up = jnp.dot(rows, up_ref[0], preferred_element_type=F32)
        act = (gate * jax.nn.sigmoid(gate) * up).astype(BF16)
        out_ref[0] = jnp.dot(act, down_ref[0], preferred_element_type=F32).astype(BF16)


def expert_ffn(counts, rows, w_gate, w_up, w_down):
    slots, padded, hidden = rows.shape
    ff = w_gate.shape[2]
    tiles = padded // ROW_TILE

    def row_map(e, r, count_ref):
        filled = lax.div(count_ref[e] + (ROW_TILE - 1), ROW_TILE)
        return e, jnp.maximum(r - (tiles - filled), 0), 0

    def weight_map(e, r, count_ref):
        return e, 0, 0

    return pl.pallas_call(
        ffn_kernel,
        out_shape=jax.ShapeDtypeStruct((slots, padded, hidden), BF16),
        grid_spec=pltpu.PrefetchScalarGridSpec(
            num_scalar_prefetch=1,
            grid=(slots, tiles),
            in_specs=[
                pl.BlockSpec((1, ROW_TILE, hidden), row_map),
                pl.BlockSpec((1, hidden, ff), weight_map),
                pl.BlockSpec((1, hidden, ff), weight_map),
                pl.BlockSpec((1, ff, hidden), weight_map),
            ],
            out_specs=pl.BlockSpec((1, ROW_TILE, hidden), row_map),
        ),
        compiler_params=pltpu.CompilerParams(
            dimension_semantics=("arbitrary", "arbitrary"), vmem_limit_bytes=58 * 1024 * 1024),
        cost_estimate=pl.CostEstimate(
            flops=3 * slots * padded * hidden * ff, bytes_accessed=6 * slots * hidden * ff,
            transcendentals=0),
        name="expert_ffn",
    )(counts, rows, w_gate, w_up, w_down)


def combine_kernel(slots, window, start_ref, count_ref, meta_ref, rows_ref, out_ref):
    source = pl.program_id(0)
    tokens = meta_ref.shape[0]
    padded = rows_ref.shape[1]
    lane = lax.broadcasted_iota(jnp.int32, (tokens, window), 1)
    sub = lax.broadcasted_iota(jnp.int32, (window, 1), 0)
    meta = meta_ref[...]
    for e in range(slots):
        first = lax.div(start_ref[source * slots + e], 16) * 16
        first = pl.multiple_of(jnp.minimum(first, padded - window), 16)
        rows = rows_ref[e, pl.ds(first, window), :]
        rows = jnp.where(sub + first < count_ref[e], rows, jnp.zeros_like(rows))
        wanted = meta[:, e:e + 1].astype(jnp.int32) - first
        pick = (lane == wanted).astype(F32).astype(BF16)
        term = meta[:, slots + e:slots + e + 1] * jnp.dot(pick, rows, preferred_element_type=F32)
        if e == 0:
            out_ref[0] = term
        else:
            out_ref[0] += term


def combine(starts, counts, meta, rows, window, sources):
    slots, padded, hidden = rows.shape
    tokens = meta.shape[0] // sources
    return pl.pallas_call(
        functools.partial(combine_kernel, slots, window),
        out_shape=jax.ShapeDtypeStruct((sources, tokens, hidden), F32),
        grid_spec=pltpu.PrefetchScalarGridSpec(
            num_scalar_prefetch=2,
            grid=(sources,),
            in_specs=[
                pl.BlockSpec((tokens, meta.shape[1]), lambda s, *_: (s, 0)),
                pl.BlockSpec((slots, padded, hidden), lambda s, *_: (0, 0, 0),
                             pipeline_mode=pl.Buffered(1)),
            ],
            out_specs=pl.BlockSpec((1, tokens, hidden), lambda s, *_: (s, 0, 0)),
        ),
        compiler_params=pltpu.CompilerParams(
            dimension_semantics=("arbitrary",), vmem_limit_bytes=48 * 1024 * 1024),
        cost_estimate=pl.CostEstimate(
            flops=2 * sources * tokens * slots * 256 * hidden,
            bytes_accessed=4 * sources * tokens * hidden, transcendentals=0),
        name="combine",
    )(starts, counts, meta, rows)


def solution(mesh):
    group_size = mesh.shape['ep']

    def device_block(hidden_in, topk_idx, norm_gain, w_router, w_sgate, s_gate, s_up, s_down, w_gate, w_up, w_down):
        tok_dev, hidden = hidden_in.shape
        top_k = topk_idx.shape[1]
        experts = w_router.shape[1]
        slots = w_gate.shape[0]
        capacity = (5 * tok_dev * group_size * top_k + 4 * experts - 1) // (4 * experts)
        local_max = (2 * tok_dev * top_k + experts - 1) // experts
        padded = -(-capacity // ROW_TILE) * ROW_TILE
        window = -(-local_max // 16) * 16 + 16
        bounds = [tok_dev * sum(SPLIT[:c]) // sum(SPLIT) for c in range(len(SPLIT) + 1)]
        my_rank = lax.axis_index('ep')

        normed, inv_rms = rms_norm(hidden_in, norm_gain)
        gain = norm_gain.astype(F32)[None]
        gathered = [lax.all_gather(hidden_in[lo:hi], 'ep', tiled=True) for lo, hi in zip(bounds, bounds[1:])]

        logits = lax.dot_general(w_router, normed, (((0,), (1,)), ((), ())), preferred_element_type=F32)
        probs = jax.nn.softmax(logits, axis=0)
        ids = topk_idx.T
        ids_f32 = ids.astype(F32)
        gates = jnp.sum(jnp.where(ids[:, None, :] == jnp.arange(experts)[None, :, None], probs[None], 0.0), axis=1)
        route = lax.all_gather(jnp.concatenate([ids_f32, gates, inv_rms.T], axis=0), 'ep')
        all_ids, all_gates, all_inv = route[:, :top_k], route[:, top_k:2 * top_k], route[:, 2 * top_k:]

        my_slots = (my_rank * slots + jnp.arange(slots)).astype(F32)
        match = all_ids[None] == my_slots[:, None, None, None]
        hit = jnp.sum(match.astype(F32), axis=2)
        gate = jnp.sum(jnp.where(match, all_gates[None], 0.0), axis=2)
        order = exclusive_count(hit.reshape(slots, group_size * tok_dev)).reshape(hit.shape)
        kept = jnp.where(order < capacity, hit, 0.0)

        partial_sums = []
        for c, (lo, hi) in enumerate(zip(bounds, bounds[1:])):
            part = hi - lo
            kept_c = kept[:, :, lo:hi].reshape(slots, group_size * part)
            gate_c = gate[:, :, lo:hi].reshape(slots, group_size * part)
            place = exclusive_count(kept_c)
            place = jnp.where(kept_c > 0, place, -1.0)
            per_source = jnp.sum(kept_c.reshape(slots, group_size, part), axis=2).astype(jnp.int32)
            counts = jnp.sum(per_source, axis=1)
            starts = (jnp.cumsum(per_source, axis=1) - per_source).T.reshape(-1)
            meta = jnp.concatenate([place, gate_c], axis=0).T
            seats = jnp.concatenate(
                [place.reshape(slots, group_size, part).transpose(1, 0, 2), all_inv[:, :, lo:hi]], axis=1)
            rows = pack_rows(starts, seats, gain, gathered[c], slots, padded, window, group_size)
            results = expert_ffn(counts, rows, w_gate, w_up, w_down)
            partial = combine(starts, counts, meta, results, window, group_size)
            partial_sums.append(partial.reshape(group_size * part, hidden))
        routed = [lax.psum_scatter(p, 'ep', scatter_dimension=0, tiled=True) for p in partial_sums]
        shared_in, _ = lax.optimization_barrier((normed, partial_sums[0]))
        shared_val = shared_expert(shared_in, w_sgate, s_gate, s_up, s_down)
        base = lax.optimization_barrier(hidden_in.astype(F32) + shared_val)
        return (base + jnp.concatenate(routed, axis=0)).astype(BF16)

    row_spec = P(('dp', 'ep'), None)
    full_spec = P(None, None)
    slot_spec = P('ep', None, None)
    in_specs = (row_spec, row_spec, P(None), full_spec, full_spec, full_spec, full_spec, full_spec,
                slot_spec, slot_spec, slot_spec)
    return jax.shard_map(device_block, mesh=mesh, in_specs=in_specs, out_specs=row_spec, check_vma=False)
```
